32 devices in a mesh: expert: 4 (over x, core), fsdp: 8 (over z, y).
Axes of the slice: x: 2, y: 2, z: 4, core: 2. Of those that a mesh axis runs over, the one named last changes fastest.
Arguments:
- momentum: float32 [4, 7168, 1024], P(None, ('fsdp', 'expert')), may hold values from -6 to 6
- spectral_sq: float32 [4], P('expert'), may hold values from 10752 to 35840
Outputs:
- update: bfloat16 [4, 7168, 1024], P(None, ('fsdp', 'expert'))
The draws below stay inside these ranges and needn't reach their ends.
All inputs are finite; a program needn't handle non-finite values.
Results may differ from the reference program's by a relative error of at most 0.0064.
Values may be sent and summed in bfloat16 or wider, within the bound.
No kernel may reach another device: no remote copies, remote signals or barrier semaphores. Data moves between devices by JAX's collectives and lax.ppermute only.
A program may use at most 64 MiB of HBM per device.

```python
import math
import jax
import jax.numpy as jnp
from jax import lax

C = 7168
R = 1024
EXPERTS = 4


def draw_momentum(key, part):
    first_key = jax.random.fold_in(key, 11)
    values = jax.random.normal(first_key, (EXPERTS, C, R), jnp.float32)
    return jnp.clip(values, -6.0, 6.0)


def block_levels(key, dims, cuts, smallest, top_value):
    loudness = 1.0
    for position, shards_of in cuts:
        steps = jax.random.uniform(jax.random.fold_in(jax.random.fold_in(key, 6), position), (shards_of,), jnp.float32, smallest / len(cuts), top_value / len(cuts))
        loudness = loudness * jnp.repeat(jnp.exp(steps), dims[position] // shards_of).reshape((-1,) + (1,) * (len(dims) - 1 - position))
    return loudness


def setup_inputs(seed: int = 0) -> dict:
    arg_keys = jax.random.split(jax.random.key(seed), 3)
    momentum = draw_momentum(jax.random.fold_in(arg_keys[2], 71), 0)
    spectral_sq = jnp.clip(jnp.exp(math.log(35840.0) - 1.2039728 * jax.random.uniform(arg_keys[1], (EXPERTS,), jnp.float32) ** block_levels(arg_keys[1], (EXPERTS,), ((0, 4),), -0.2, 0.2)), 10752.0, 35840.0)
    return dict(momentum=momentum, spectral_sq=spectral_sq)


coef_a = 3.4445
coef_b = -4.775
coef_c = 2.0315

def one_matrix(pieces):
    matrix, square = pieces
    scaled = (matrix / jnp.sqrt(square)).astype(jnp.bfloat16)
    gram_sum = jnp.dot(scaled.T, scaled, preferred_element_type=jnp.float32)
    rounded = gram_sum.astype(jnp.bfloat16)
    product = jnp.dot(rounded, rounded, preferred_element_type=jnp.float32)
    polynomial = (coef_b * rounded.astype(jnp.float32) + coef_c * product).astype(jnp.bfloat16)
    update = coef_a * scaled.astype(jnp.float32) + jnp.dot(scaled, polynomial, preferred_element_type=jnp.float32)
    return (update * jnp.sqrt(jnp.float32(C))).astype(jnp.bfloat16)

def reference(momentum, spectral_sq):
    return lax.map(one_matrix, (momentum, spectral_sq))
```

```python
import functools

import jax
import jax.numpy as jnp
from jax import lax
from jax.experimental import pallas as pl
from jax.experimental.pallas import tpu as pltpu
from jax.sharding import PartitionSpec as P

coef_a = 3.4445
coef_b = -4.775
coef_c = 2.0315

TILE = 128
PAD = 16
VMEM = pl.BlockSpec(memory_space=pltpu.VMEM)
SMEM = pl.BlockSpec(memory_space=pltpu.SMEM)


def block_table(tiles):
    table = [(i, j) for i in range(tiles) for j in range(i + 1, tiles)]
    return table + [(i, i) for i in range(0, tiles, 2)]


def contract_rows(left, right):
    return lax.dot_general(
        left, right, (((0,), (0,)), ((), ())), preferred_element_type=jnp.float32
    )


def tile_iota():
    rows = lax.broadcasted_iota(jnp.int32, (TILE, TILE), 0)
    cols = lax.broadcasted_iota(jnp.int32, (TILE, TILE), 1)
    return rows, cols


def gram_kernel(core_ref, inverse_ref, *refs):
    *row_refs, keep_ref, send_ref, packed = refs
    order = row_refs[0].shape[1]
    tiles = order // TILE
    table = block_table(tiles)
    place = {pair: index for index, pair in enumerate(table)}
    half_rows = packed.shape[1] - PAD
    per_half = half_rows // TILE
    inverse = inverse_ref[0]
    rows, cols = tile_iota()

    def put(index, value):
        half, slot = divmod(index, per_half)
        packed[half, pl.ds(slot * TILE, TILE), :] = value

    diagonals = []
    for panel in range(tiles // 2):
        start = 2 * panel * TILE
        total = None
        for ref in row_refs:
            part = contract_rows(ref[:, start : start + 2 * TILE], ref[:, start:])
            total = part if total is None else total + part
        total = total * inverse
        for side in range(2):
            i = 2 * panel + side
            for j in range(i + 1, tiles):
                at = j * TILE - start
                put(place[i, j], total[side * TILE : (side + 1) * TILE, at : at + TILE])
        first, second = total[:TILE, :TILE], total[TILE:, TILE : 2 * TILE]
        put(place[2 * panel, 2 * panel], jnp.where(cols >= rows, first, second))
        diagonals.append(jnp.sum(jnp.where(rows == cols, second, 0.0), axis=0, keepdims=True))
    tail = jnp.concatenate(
        diagonals + [jnp.zeros((PAD - len(diagonals), TILE), jnp.float32)], axis=0
    )
    for half in range(2):
        packed[half, pl.ds(half_rows, PAD), :] = tail
    core = core_ref[0]
    keep_ref[...] = packed[core]
    send_ref[...] = packed[1 - core].astype(jnp.bfloat16)


def split_kernel(place_ref, keep_ref, recv_ref, own_ref, *send_refs):
    parts = len(send_refs) + 1
    size = own_ref.shape[0] - PAD
    place = place_ref[0]
    tail = keep_ref[pl.ds(parts * size, PAD), :] + recv_ref[pl.ds(parts * size, PAD), :].astype(
        jnp.float32
    )
    for mask in range(parts):
        at = pl.ds(pl.multiple_of((place ^ mask) * size, size), size)
        total = keep_ref[at, :] + recv_ref[at, :].astype(jnp.float32)
        out = own_ref if mask == 0 else send_refs[mask - 1]
        out[pl.ds(0, size), :] = total.astype(out.dtype)
        out[pl.ds(size, PAD), :] = tail.astype(out.dtype)


def polynomial_kernel(place_ref, *refs):
    *shard_refs, out_ref, packed, gram = refs
    parts = len(shard_refs) // 2
    size = shard_refs[0].shape[0] - PAD
    order = out_ref.shape[0]
    table = block_table(order // TILE)
    place, core = place_ref[0], place_ref[1]
    for side in range(2):
        for mask in range(parts):
            at = ((core ^ side) * parts + (place ^ mask)) * size
            packed[pl.ds(pl.multiple_of(at, size), size), :] = shard_refs[side * parts + mask][
                pl.ds(0, size), :
            ]
    tail = shard_refs[0][pl.ds(size, PAD), :].astype(jnp.float32)
    rows, cols = tile_iota()
    for index, (i, j) in enumerate(table):
        tile = packed[pl.ds(index * TILE, TILE), :]
        if i != j:
            gram[pl.ds(i * TILE, TILE), pl.ds(j * TILE, TILE)] = tile
            gram[pl.ds(j * TILE, TILE), pl.ds(i * TILE, TILE)] = tile.T
        else:
            wide = tile.astype(jnp.float32)
            flipped = wide.T
            first = jnp.where(cols >= rows, wide, flipped)
            diagonal = jnp.broadcast_to(tail[i // 2 : i // 2 + 1, :], (TILE, TILE))
            second = jnp.where(rows > cols, wide, jnp.where(rows < cols, flipped, diagonal))
            a, b = pl.ds(i * TILE, TILE), pl.ds((i + 1) * TILE, TILE)
            gram[a, a] = first.astype(jnp.bfloat16)
            gram[b, b] = second.astype(jnp.bfloat16)
    step = 2 * TILE
    for at in range(0, order, step):
        square = jnp.dot(gram[pl.ds(at, step), :], gram[...], preferred_element_type=jnp.float32)
        out_ref[pl.ds(at, step), :] = (
            coef_b * gram[pl.ds(at, step), :].astype(jnp.float32) + coef_c * square
        ).astype(jnp.bfloat16)


def call(kernel, name, out, in_specs, scratch, flops):
    return pl.pallas_call(
        kernel,
        name=name,
        out_shape=out,
        in_specs=in_specs,
        out_specs=jax.tree.map(lambda _: VMEM, out),
        scratch_shapes=scratch,
        cost_estimate=pl.CostEstimate(flops=flops, bytes_accessed=4 << 20, transcendentals=0),
        compiler_params=pltpu.CompilerParams(vmem_limit_bytes=40 << 20),
    )


def on_device(experts, pieces, height, momentum, spectral_sq):
    axes = ("expert", "fsdp")
    e, f = lax.axis_index("expert"), lax.axis_index("fsdp")
    core, low, place = e & 1, f & 1, f >> 1
    own = (e & ~1) + low
    parts = pieces // 2
    count, order = momentum.shape[1:]

    def exchange(value, e_mask, f_mask):
        pairs = [
            (k * pieces + i, (k ^ e_mask) * pieces + (i ^ f_mask))
            for k in range(experts)
            for i in range(pieces)
        ]
        return lax.ppermute(value, axes, pairs)

    def other_core(value):
        return exchange(value, 1, 0)

    def to_expert(value, mask):
        return exchange(value, mask & ~1, mask & 1)

    def to_place(value, mask):
        return exchange(value, 0, mask << 1)

    def rows_of(mask):
        block = lax.dynamic_index_in_dim(momentum, own ^ mask, 0, keepdims=False)
        return block.astype(jnp.bfloat16)

    masks = list(range(experts - 1, 0, -1))
    received = {mask: to_expert(rows_of(mask), mask) for mask in masks}
    received[0] = rows_of(0)
    square = jnp.where(core == low, spectral_sq, other_core(spectral_sq))
    blocks = [received[mask] for mask in range(experts)]
    gram_rows = blocks if count % 16 == 0 else [jnp.concatenate(blocks, 0)]

    tiles = order // TILE
    half = len(block_table(tiles)) * TILE // 2
    f32, bf16 = jnp.float32, jnp.bfloat16
    shape = jax.ShapeDtypeStruct
    keep, send = call(
        gram_kernel,
        "gram",
        (shape((half + PAD, TILE), f32), shape((half + PAD, TILE), bf16)),
        [SMEM, SMEM] + [VMEM] * len(gram_rows),
        [pltpu.VMEM((2, half + PAD, TILE), f32)],
        experts * count * order * order,
    )(core.reshape(1), 1.0 / square, *gram_rows)
    size = half // parts
    own_part, *sends = call(
        split_kernel,
        "split",
        (shape((size + PAD, TILE), f32),) + (shape((size + PAD, TILE), bf16),) * (parts - 1),
        [SMEM, VMEM, VMEM],
        [],
        half * TILE,
    )(place.reshape(1), keep, other_core(send))
    order_of = list(range(parts - 1, 0, -1))
    arrived = {mask: to_place(sends[mask - 1], mask) for mask in order_of}
    total = own_part
    for mask in range(1, parts):
        total = total + arrived[mask].astype(f32)
    shard = total.astype(bf16)
    shards = {mask: to_place(shard, mask) for mask in order_of}
    shards[0] = shard
    here = [shards[mask] for mask in range(parts)]
    there = [other_core(value) for value in here]
    polynomial = call(
        polynomial_kernel,
        "polynomial",
        shape((order, order), bf16),
        [SMEM] + [VMEM] * (2 * parts),
        [pltpu.VMEM((2 * half, TILE), bf16), pltpu.VMEM((order, order), bf16)],
        2 * order**3,
    )(jnp.stack([place, core]), *here, *there)
    scale = (jnp.sqrt(jnp.float32(height)) * lax.rsqrt(square))[0]

    def update_of(mask):
        rows = received[mask]
        product = jnp.dot(rows, polynomial, preferred_element_type=f32)
        return ((coef_a * rows.astype(f32) + product) * scale).astype(bf16)

    back = {mask: to_expert(update_of(mask), mask) for mask in masks}
    back[0] = update_of(0)
    result = jnp.zeros((experts, count, order), bf16)
    for mask in [0] + masks[::-1]:
        result = lax.dynamic_update_index_in_dim(result, back[mask], own ^ mask, 0)
    return result


def solution(mesh):
    experts, pieces = mesh.shape["expert"], mesh.shape["fsdp"]

    def run(momentum, spectral_sq):
        body = functools.partial(on_device, experts, pieces, momentum.shape[1])
        return jax.shard_map(
            body,
            mesh=mesh,
            in_specs=(P(None, ("fsdp", "expert"), None), P("expert")),
            out_specs=P(None, ("fsdp", "expert"), None),
            check_vma=False,
        )(momentum, spectral_sq)

    return run
```

```python
import jax
import jax.numpy as jnp
from jax import lax
from jax.experimental import pallas as pl
from jax.experimental.pallas import tpu as pltpu
from jax.sharding import PartitionSpec as P

coef_a = 3.4445
coef_b = -4.775
coef_c = 2.0315

LIMIT = 12 << 20
TILE = 128
PAD = 16
VMEM = pl.BlockSpec(memory_space=pltpu.VMEM)
SMEM = pl.BlockSpec(memory_space=pltpu.SMEM)


def block_table(tiles):
    table = [(i, j) for i in range(tiles) for j in range(i + 1, tiles)]
    return table + [(i, i) for i in range(0, tiles, 2)]


def contract_rows(left, right):
    return lax.dot_general(
        left, right, (((0,), (0,)), ((), ())), preferred_element_type=jnp.float32
    )


def tile_iota():
    rows = lax.broadcasted_iota(jnp.int32, (TILE, TILE), 0)
    cols = lax.broadcasted_iota(jnp.int32, (TILE, TILE), 1)
    return rows, cols


def gram_kernel(core_ref, *refs):
    *row_refs, keep_ref, send_ref, packed = refs
    order = row_refs[0].shape[1]
    tiles = order // TILE
    table = block_table(tiles)
    place = {pair: index for index, pair in enumerate(table)}
    half_rows = packed.shape[1] - PAD
    per_half = half_rows // TILE
    rows, cols = tile_iota()

    def put(index, value):
        half, slot = divmod(index, per_half)
        packed[half, pl.ds(slot * TILE, TILE), :] = value

    diagonals = []
    for panel in range(tiles // 2):
        start = 2 * panel * TILE
        total = None
        for ref in row_refs:
            part = contract_rows(ref[:, start : start + 2 * TILE], ref[:, start:])
            total = part if total is None else total + part
        for side in range(2):
            i = 2 * panel + side
            for j in range(i + 1, tiles):
                at = j * TILE - start
                put(place[i, j], total[side * TILE : (side + 1) * TILE, at : at + TILE])
        first, second = total[:TILE, :TILE], total[TILE:, TILE : 2 * TILE]
        put(place[2 * panel, 2 * panel], jnp.where(cols >= rows, first, second))
        diagonals.append(jnp.sum(jnp.where(rows == cols, second, 0.0), axis=0, keepdims=True))
    tail = jnp.concatenate(
        diagonals + [jnp.zeros((PAD - len(diagonals), TILE), jnp.float32)], axis=0
    )
    for half in range(2):
        packed[half, pl.ds(half_rows, PAD), :] = tail
    core = core_ref[0]
    keep_ref[...] = packed[core]
    send_ref[...] = packed[1 - core].astype(jnp.bfloat16)


def split_kernel(place_ref, keep_ref, recv_ref, own_ref, *send_refs):
    parts = len(send_refs) + 1
    size = own_ref.shape[0] - PAD
    place = place_ref[0]
    tail = keep_ref[pl.ds(parts * size, PAD), :] + recv_ref[pl.ds(parts * size, PAD), :].astype(
        jnp.float32
    )
    for mask in range(parts):
        at = pl.ds(pl.multiple_of((place ^ mask) * size, size), size)
        total = keep_ref[at, :] + recv_ref[at, :].astype(jnp.float32)
        out = own_ref if mask == 0 else send_refs[mask - 1]
        out[pl.ds(0, size), :] = total.astype(out.dtype)
        out[pl.ds(size, PAD), :] = tail.astype(out.dtype)


def total_kernel(*refs):
    *part_refs, out_ref = refs
    total = part_refs[0][...]
    for ref in part_refs[1:]:
        total = total + ref[...].astype(jnp.float32)
    out_ref[...] = total.astype(jnp.bfloat16)


def round_kernel(inverse_ref, *refs):
    *part_refs, out_ref, shard_ref = refs
    total = part_refs[0][...]
    for ref in part_refs[1:]:
        total = total + ref[...].astype(jnp.float32)
    rounded = (total * inverse_ref[0]).astype(jnp.bfloat16)
    out_ref[...] = rounded
    shard_ref[...] = rounded[: shard_ref.shape[0]]


def unpack(place_ref, tail_ref, shard_refs, packed, gram):
    parts = len(shard_refs) // 2
    tiles = gram.shape[0] // TILE
    table = block_table(tiles)
    size = len(table) * TILE // len(shard_refs)
    place, core = place_ref[0], place_ref[1]
    for side in range(2):
        for mask in range(parts):
            at = ((core ^ side) * parts + (place ^ mask)) * size
            packed[pl.ds(pl.multiple_of(at, size), size), :] = shard_refs[side * parts + mask][
                pl.ds(0, size), :
            ]
    tail = tail_ref[pl.ds(size, PAD), :].astype(jnp.float32)
    rows, cols = tile_iota()
    for index, (i, j) in enumerate(table):
        tile = packed[pl.ds(index * TILE, TILE), :]
        if i != j:
            gram[pl.ds(i * TILE, TILE), pl.ds(j * TILE, TILE)] = tile
            gram[pl.ds(j * TILE, TILE), pl.ds(i * TILE, TILE)] = tile.T
        else:
            wide = tile.astype(jnp.float32)
            flipped = wide.T
            first = jnp.where(cols >= rows, wide, flipped)
            diagonal = jnp.broadcast_to(tail[i // 2 : i // 2 + 1, :], (TILE, TILE))
            second = jnp.where(rows > cols, wide, jnp.where(rows < cols, flipped, diagonal))
            a, b = pl.ds(i * TILE, TILE), pl.ds((i + 1) * TILE, TILE)
            gram[a, a] = first.astype(jnp.bfloat16)
            gram[b, b] = second.astype(jnp.bfloat16)


def update_rows(scale_ref, row_ref, gram, out_ref, inner):
    product = jnp.dot(row_ref[...], gram[...], preferred_element_type=jnp.float32)
    inner[...] = (coef_b * row_ref[...].astype(jnp.float32) + coef_c * product).astype(jnp.bfloat16)
    product = jnp.dot(inner[...], gram[...], preferred_element_type=jnp.float32)
    out_ref[...] = (
        (coef_a * row_ref[...].astype(jnp.float32) + product) * scale_ref[0]
    ).astype(jnp.bfloat16)


def finish_kernel(place_ref, scale_ref, tail_ref, row_ref, *refs):
    *shard_refs, gram, out_ref, packed, inner = refs
    unpack(place_ref, tail_ref, shard_refs, packed, gram)
    update_rows(scale_ref, row_ref, gram, out_ref, inner)


def far_kernel(place_ref, scale_ref, tail_ref, row_ref, *refs):
    *shard_refs, out_ref, packed, inner, gram = refs
    unpack(place_ref, tail_ref, shard_refs, packed, gram)
    update_rows(scale_ref, row_ref, gram, out_ref, inner)


def cut_kernel(whole_ref, out_ref):
    out_ref[...] = whole_ref[pl.ds(0, out_ref.shape[0]), :]


def update_kernel(scale_ref, gram, row_ref, out_ref, inner):
    update_rows(scale_ref, row_ref, gram, out_ref, inner)


def place_kernel(place_ref, *refs):
    *block_refs, out_ref, sems = refs
    copies = [
        pltpu.make_async_copy(block, out_ref.at[place_ref[mask]], sems.at[mask])
        for mask, block in enumerate(block_refs)
    ]
    for copy in copies:
        copy.start()
    for copy in copies:
        copy.wait()


def call(kernel, out, in_specs, scratch, flops):
    return pl.pallas_call(
        kernel,
        out_shape=out,
        in_specs=in_specs,
        out_specs=jax.tree.map(lambda _: VMEM, out),
        scratch_shapes=scratch,
        cost_estimate=pl.CostEstimate(flops=int(flops), bytes_accessed=4 << 20, transcendentals=0),
        compiler_params=pltpu.CompilerParams(vmem_limit_bytes=LIMIT),
    )


def on_device(experts, pieces, height, momentum, spectral_sq):
    axes = ("expert", "fsdp")
    e, f = lax.axis_index("expert"), lax.axis_index("fsdp")
    core, low, place = e & 1, f & 1, f >> 1
    own = (e & ~1) + low
    parts = pieces // 2
    count, order = momentum.shape[1:]

    def exchange(value, e_mask, f_mask):
        pairs = [
            (k * pieces + i, (k ^ e_mask) * pieces + (i ^ f_mask))
            for k in range(experts)
            for i in range(pieces)
        ]
        return lax.ppermute(value, axes, pairs)

    def other_core(value):
        return exchange(value, 1, 0)

    def to_expert(value, mask):
        return exchange(value, mask & ~1, mask & 1)

    def to_place(value, mask):
        return exchange(value, 0, mask << 1)

    f32, bf16 = jnp.float32, jnp.bfloat16
    shape = jax.ShapeDtypeStruct
    tiles = order // TILE
    half = len(block_table(tiles)) * TILE // 2
    size = half // parts
    corner = jnp.stack([place, core])
    places = list(range(parts - 1, 0, -1))
    far = experts - 1
    near = list(range(1, far))

    def column_sum(rows):
        rows = rows if count % PAD == 0 else [jnp.concatenate(rows, 0)]
        keep, send = call(
            gram_kernel,
            (shape((half + PAD, TILE), f32), shape((half + PAD, TILE), bf16)),
            [SMEM] + [VMEM] * len(rows),
            [pltpu.VMEM((2, half + PAD, TILE), f32)],
            len(rows) * rows[0].shape[0] * order * order,
        )(core.reshape(1), *rows)
        swapped = other_core(send)
        own_part, *sends = call(
            split_kernel,
            (shape((size + PAD, TILE), f32),) + (shape((size + PAD, TILE), bf16),) * (parts - 1),
            [SMEM, VMEM, VMEM],
            [],
            half * TILE,
        )(place.reshape(1), keep, swapped)
        arrived = []
        for mask in places:
            arrived.append(to_place(sends[mask - 1], mask))
        return [own_part] + arrived

    def gather(shard):
        here = {0: shard}
        for mask in places:
            here[mask] = to_place(shard, mask)
        there = []
        for mask in range(parts):
            there.append(other_core(here[mask]))
        return [here[mask] for mask in range(parts)] + there

    def finish(name, scale, tail, rows, shards):
        gram_shape = (order, order)
        rows_shape = shape((count, order), bf16)
        keep = name == "near"
        return call(
            finish_kernel if keep else far_kernel,
            (shape(gram_shape, bf16), rows_shape) if keep else rows_shape,
            [SMEM, SMEM] + [VMEM] * (2 + len(shards)),
            [pltpu.VMEM((2 * half, TILE), bf16), pltpu.VMEM((count, order), bf16)]
            + ([] if keep else [pltpu.VMEM(gram_shape, bf16)]),
            4 * count * order * order,
        )(corner, scale, tail, rows, *shards)

    local = [
        lax.dynamic_index_in_dim(momentum, own ^ mask, 0, keepdims=False).astype(bf16)
        for mask in range(experts)
    ]
    received = {0: local[0]}
    for mask in near:
        received[mask] = to_expert(local[mask], mask)
    far_parts = column_sum([local[far]])
    square = jnp.where(core == low, spectral_sq, other_core(spectral_sq))
    far_square = to_expert(square, far)
    far_sum = call(
        total_kernel,
        shape((size + PAD, TILE), bf16),
        [VMEM] * len(far_parts),
        [],
        size * TILE * parts,
    )(*far_parts)
    far_sum = to_expert(far_sum, far)
    near_parts = column_sum([received[mask] for mask in [0] + near])
    rounded, shard = call(
        round_kernel,
        (shape((size + PAD, TILE), bf16), shape((size, TILE), bf16)),
        [SMEM] + [VMEM] * (len(near_parts) + 1),
        [],
        size * TILE * parts,
    )(1.0 / square, *near_parts, far_sum)
    shards = gather(shard)
    far_rounded = to_expert(rounded, far)
    far_shard = call(cut_kernel, shape((size, TILE), bf16), [VMEM], [], size * TILE)(far_rounded)
    far_shards = gather(far_shard)
    height_root = jnp.sqrt(jnp.float32(height))
    scale = height_root * lax.rsqrt(square)
    far_scale = height_root * lax.rsqrt(far_square)

    back = {}
    first = near[0]
    gram, back[first] = finish("near", scale, rounded, received[first], shards)
    for mask in near[1:] + [0]:
        back[mask] = call(
            update_kernel,
            shape((count, order), bf16),
            [SMEM, VMEM, VMEM],
            [pltpu.VMEM((count, order), bf16)],
            4 * count * order * order,
        )(scale, gram, received[mask])
    for mask in near:
        back[mask] = to_expert(back[mask], mask)
    back[far] = finish("far", far_scale, far_rounded, local[far], far_shards)
    if count % PAD:
        result = jnp.zeros((experts, count, order), bf16)
        for mask in range(experts):
            result = lax.dynamic_update_index_in_dim(result, back[mask], own ^ mask, 0)
        return result
    return pl.pallas_call(
        place_kernel,
        name="place",
        out_shape=shape((experts, count, order), bf16),
        in_specs=[SMEM] + [VMEM] * experts,
        out_specs=pl.BlockSpec(memory_space=pltpu.HBM),
        scratch_shapes=[pltpu.SemaphoreType.DMA((experts,))],
        compiler_params=pltpu.CompilerParams(vmem_limit_bytes=LIMIT),
    )(own ^ jnp.arange(experts, dtype=jnp.int32), *[back[mask] for mask in range(experts)])


def solution(mesh):
    experts, pieces = mesh.shape["expert"], mesh.shape["fsdp"]

    def body(momentum, spectral_sq):
        height = momentum.shape[1] * experts * pieces
        return on_device(experts, pieces, height, momentum, spectral_sq)

    return jax.shard_map(
        body,
        mesh=mesh,
        in_specs=(P(None, ("fsdp", "expert"), None), P("expert")),
        out_specs=P(None, ("fsdp", "expert"), None),
        check_vma=False,
    )
```

```python
import functools

import jax
import jax.numpy as jnp
from jax import lax
from jax.experimental import pallas as pl
from jax.experimental.pallas import tpu as pltpu
from jax.sharding import PartitionSpec as P

coef_a = 3.4445
coef_b = -4.775
coef_c = 2.0315

LIMIT = 12 << 20
TILE = 128
PAD = 16
VMEM = pl.BlockSpec(memory_space=pltpu.VMEM)
SMEM = pl.BlockSpec(memory_space=pltpu.SMEM)


def block_table(tiles):
    table = [(i, j) for i in range(tiles) for j in range(i + 1, tiles)]
    return table + [(i, i) for i in range(0, tiles, 2)]


def contract_rows(left, right):
    return lax.dot_general(
        left, right, (((0,), (0,)), ((), ())), preferred_element_type=jnp.float32
    )


def tile_iota():
    rows = lax.broadcasted_iota(jnp.int32, (TILE, TILE), 0)
    cols = lax.broadcasted_iota(jnp.int32, (TILE, TILE), 1)
    return rows, cols


def gram_kernel(core_ref, *refs):
    *row_refs, keep_ref, send_ref, packed = refs
    order = row_refs[0].shape[1]
    tiles = order // TILE
    table = block_table(tiles)
    place = {pair: index for index, pair in enumerate(table)}
    half_rows = packed.shape[1] - PAD
    per_half = half_rows // TILE
    rows, cols = tile_iota()

    def put(index, value):
        half, slot = divmod(index, per_half)
        packed[half, pl.ds(slot * TILE, TILE), :] = value

    diagonals = []
    for panel in range(tiles // 2):
        start = 2 * panel * TILE
        total = None
        for ref in row_refs:
            part = contract_rows(ref[:, start : start + 2 * TILE], ref[:, start:])
            total = part if total is None else total + part
        for side in range(2):
            i = 2 * panel + side
            for j in range(i + 1, tiles):
                at = j * TILE - start
                put(place[i, j], total[side * TILE : (side + 1) * TILE, at : at + TILE])
        first, second = total[:TILE, :TILE], total[TILE:, TILE : 2 * TILE]
        put(place[2 * panel, 2 * panel], jnp.where(cols >= rows, first, second))
        diagonals.append(jnp.sum(jnp.where(rows == cols, second, 0.0), axis=0, keepdims=True))
    tail = jnp.concatenate(
        diagonals + [jnp.zeros((PAD - len(diagonals), TILE), jnp.float32)], axis=0
    )
    for half in range(2):
        packed[half, pl.ds(half_rows, PAD), :] = tail
    core = core_ref[0]
    keep_ref[...] = packed[core]
    send_ref[...] = packed[1 - core].astype(jnp.bfloat16)


def split_kernel(place_ref, keep_ref, recv_ref, own_ref, *send_refs):
    parts = len(send_refs) + 1
    size = own_ref.shape[0] - PAD
    place = place_ref[0]
    tail = keep_ref[pl.ds(parts * size, PAD), :] + recv_ref[pl.ds(parts * size, PAD), :].astype(
        jnp.float32
    )
    for mask in range(parts):
        at = pl.ds(pl.multiple_of((place ^ mask) * size, size), size)
        total = keep_ref[at, :] + recv_ref[at, :].astype(jnp.float32)
        out = own_ref if mask == 0 else send_refs[mask - 1]
        out[pl.ds(0, size), :] = total.astype(out.dtype)
        out[pl.ds(size, PAD), :] = tail.astype(out.dtype)


def total_kernel(*refs):
    *part_refs, out_ref = refs
    total = part_refs[0][...]
    for ref in part_refs[1:]:
        total = total + ref[...].astype(jnp.float32)
    out_ref[...] = total.astype(jnp.bfloat16)


def round_kernel(inverse_ref, *refs):
    *part_refs, out_ref, shard_ref = refs
    total = part_refs[0][...]
    for ref in part_refs[1:]:
        total = total + ref[...].astype(jnp.float32)
    rounded = (total * inverse_ref[0]).astype(jnp.bfloat16)
    out_ref[...] = rounded
    shard_ref[...] = rounded[: shard_ref.shape[0]]


def unpack(place_ref, tail_ref, shard_refs, packed, gram):
    parts = len(shard_refs) // 2
    tiles = gram.shape[0] // TILE
    table = block_table(tiles)
    size = len(table) * TILE // len(shard_refs)
    place, core = place_ref[0], place_ref[1]
    for side in range(2):
        for mask in range(parts):
            at = ((core ^ side) * parts + (place ^ mask)) * size
            packed[pl.ds(pl.multiple_of(at, size), size), :] = shard_refs[side * parts + mask][
                pl.ds(0, size), :
            ]
    tail = tail_ref[pl.ds(size, PAD), :].astype(jnp.float32)
    rows, cols = tile_iota()
    for index, (i, j) in enumerate(table):
        tile = packed[pl.ds(index * TILE, TILE), :]
        if i != j:
            gram[pl.ds(i * TILE, TILE), pl.ds(j * TILE, TILE)] = tile
            gram[pl.ds(j * TILE, TILE), pl.ds(i * TILE, TILE)] = tile.T
        else:
            wide = tile.astype(jnp.float32)
            flipped = wide.T
            first = jnp.where(cols >= rows, wide, flipped)
            diagonal = jnp.broadcast_to(tail[i // 2 : i // 2 + 1, :], (TILE, TILE))
            second = jnp.where(rows > cols, wide, jnp.where(rows < cols, flipped, diagonal))
            a, b = pl.ds(i * TILE, TILE), pl.ds((i + 1) * TILE, TILE)
            gram[a, a] = first.astype(jnp.bfloat16)
            gram[b, b] = second.astype(jnp.bfloat16)


def update_rows(scale_ref, row_refs, start, gram, out_refs, rows, inner):
    size = rows.shape[0] // len(row_refs)
    for index, ref in enumerate(row_refs):
        rows[pl.ds(index * size, size), :] = ref[pl.ds(start, size), :]
    product = jnp.dot(rows[...], gram[...], preferred_element_type=jnp.float32)
    inner[...] = (coef_b * rows[...].astype(jnp.float32) + coef_c * product).astype(jnp.bfloat16)
    product = jnp.dot(inner[...], gram[...], preferred_element_type=jnp.float32)
    product = (coef_a * rows[...].astype(jnp.float32) + product) * scale_ref[0]
    for index, ref in enumerate(out_refs):
        ref[...] = product[index * size : (index + 1) * size].astype(jnp.bfloat16)


def finish_kernel(blocks, place_ref, scale_ref, tail_ref, *refs):
    row_refs, shard_refs = refs[:blocks], refs[blocks : -4 - blocks]
    gram, out_refs = refs[-4 - blocks], refs[-3 - blocks : -3]
    packed, rows, inner = refs[-3:]
    unpack(place_ref, tail_ref, shard_refs, packed, gram)
    update_rows(scale_ref, row_refs, 0, gram, out_refs, rows, inner)


def far_kernel(place_ref, scale_ref, tail_ref, row_ref, *refs):
    *shard_refs, out_ref, packed, rows, inner, gram = refs
    unpack(place_ref, tail_ref, shard_refs, packed, gram)
    update_rows(scale_ref, [row_ref], 0, gram, [out_ref], rows, inner)


def update_kernel(blocks, start, scale_ref, gram, *refs):
    row_refs, out_refs = refs[:blocks], refs[blocks:-2]
    update_rows(scale_ref, row_refs, start, gram, out_refs, *refs[-2:])


def place_kernel(moves, earlier, place_ref, *refs):
    *block_refs, out_ref, sems = refs[earlier:]
    copies = [
        pltpu.make_async_copy(
            ref, out_ref.at[place_ref[block], pl.ds(start, ref.shape[0]), :], sems.at[index]
        )
        for index, ((block, start), ref) in enumerate(zip(moves, block_refs))
    ]
    for copy in copies:
        copy.start()
    for copy in copies:
        copy.wait()


def call(kernel, out, in_specs, scratch, flops):
    return pl.pallas_call(
        kernel,
        out_shape=out,
        in_specs=in_specs,
        out_specs=jax.tree.map(lambda _: VMEM, out),
        scratch_shapes=scratch,
        cost_estimate=pl.CostEstimate(flops=int(flops), bytes_accessed=4 << 20, transcendentals=0),
        compiler_params=pltpu.CompilerParams(vmem_limit_bytes=LIMIT),
    )


def on_device(experts, pieces, height, momentum, spectral_sq):
    axes = ("expert", "fsdp")
    e, f = lax.axis_index("expert"), lax.axis_index("fsdp")
    core, low, place = e & 1, f & 1, f >> 1
    own = (e & ~1) + low
    parts = pieces // 2
    count, order = momentum.shape[1:]

    def exchange(value, e_mask, f_mask):
        pairs = [
            (k * pieces + i, (k ^ e_mask) * pieces + (i ^ f_mask))
            for k in range(experts)
            for i in range(pieces)
        ]
        return lax.ppermute(value, axes, pairs)

    def other_core(value):
        return exchange(value, 1, 0)

    def to_expert(value, mask):
        return exchange(value, mask & ~1, mask & 1)

    def to_place(value, mask):
        return exchange(value, 0, mask << 1)

    f32, bf16 = jnp.float32, jnp.bfloat16
    shape = jax.ShapeDtypeStruct
    tiles = order // TILE
    half = len(block_table(tiles)) * TILE // 2
    size = half // parts
    corner = jnp.stack([place, core])
    where = own ^ jnp.arange(experts, dtype=jnp.int32)
    core_index, place_index = core.reshape(1), place.reshape(1)
    momentum, corner, where, core_index, place_index, same = lax.optimization_barrier(
        (momentum, corner, where, core_index, place_index, core == low)
    )
    places = list(range(parts - 1, 0, -1))
    far = experts - 1
    near = list(range(1, far))

    def column_sum(rows):
        rows = rows if count % PAD == 0 else [jnp.concatenate(rows, 0)]
        keep, send = call(
            gram_kernel,
            (shape((half + PAD, TILE), f32), shape((half + PAD, TILE), bf16)),
            [SMEM] + [VMEM] * len(rows),
            [pltpu.VMEM((2, half + PAD, TILE), f32)],
            len(rows) * rows[0].shape[0] * order * order,
        )(core_index, *rows)
        swapped = other_core(send)
        own_part, *sends = call(
            split_kernel,
            (shape((size + PAD, TILE), f32),) + (shape((size + PAD, TILE), bf16),) * (parts - 1),
            [SMEM, VMEM, VMEM],
            [],
            half * TILE,
        )(place_index, keep, swapped)
        arrived = []
        for mask in places:
            arrived.append(to_place(sends[mask - 1], mask))
        return [own_part] + arrived

    local = [
        lax.dynamic_index_in_dim(momentum, own ^ mask, 0, keepdims=False).astype(bf16)
        for mask in range(experts)
    ]
    received = {0: local[0]}
    for mask in near:
        received[mask] = to_expert(local[mask], mask)
    far_parts = column_sum([local[far]])
    square = jnp.where(same, spectral_sq, other_core(spectral_sq))
    far_square = to_expert(square, far)
    far_sum = call(
        total_kernel,
        shape((size + PAD, TILE), bf16),
        [VMEM] * len(far_parts),
        [],
        size * TILE * parts,
    )(*far_parts)
    far_sum = to_expert(far_sum, far)
    near_parts = column_sum([received[mask] for mask in [0] + near])
    rounded, shard = call(
        round_kernel,
        (shape((size + PAD, TILE), bf16), shape((size, TILE), bf16)),
        [SMEM] + [VMEM] * (len(near_parts) + 1),
        [],
        size * TILE * parts,
    )(1.0 / square, *near_parts, far_sum)
    here, far_here = {0: shard}, {}
    for mask in places:
        here[mask] = to_place(shard, mask)
    turns = gather_turns(parts)
    for mask in [0] + turns:
        if mask == turns[-1]:
            far_here[mask] = to_place(far_here[0], mask)
        else:
            far_here[mask] = to_expert(here[mask] if mask else rounded, far)
    there, far_there = {}, {}
    for mask in range(parts):
        there[mask] = other_core(here[mask])
        far_there[mask] = other_core(far_here[mask])
    shards = [kept[mask] for kept in (here, there) for mask in range(parts)]
    far_shards = [kept[mask] for kept in (far_here, far_there) for mask in range(parts)]
    height_root = jnp.sqrt(jnp.float32(height))
    scale = height_root * lax.rsqrt(square)
    far_scale = height_root * lax.rsqrt(far_square)

    lots = lots_of(count)
    lot = count // lots
    gram_shape, stack = shape((order, order), bf16), len(near) * lot
    packed_shape = pltpu.VMEM((2 * half, TILE), bf16)
    blocks = [received[mask] for mask in near]
    flops = 4 * order * order
    back = {}
    for index in range(lots):
        outs = (shape((lot, order), bf16),) * len(near)
        scratch = [pltpu.VMEM((stack, order), bf16)] * 2
        if index == 0:
            gram, *made = call(
                functools.partial(finish_kernel, len(near)),
                (gram_shape,) + outs,
                [SMEM, SMEM] + [VMEM] * (1 + len(near) + len(shards)),
                [packed_shape] + scratch,
                flops * stack,
            )(corner, scale, rounded, *blocks, *shards)
        else:
            made = call(
                functools.partial(update_kernel, len(near), index * lot),
                outs,
                [SMEM, VMEM] + [VMEM] * len(near),
                scratch,
                flops * stack,
            )(scale, gram, *blocks)
        for mask, value in zip(near, made):
            back[mask, index] = to_expert(value, mask)
    scratch = [pltpu.VMEM((count, order), bf16)] * 2
    (own_rows,) = call(
        functools.partial(update_kernel, 1, 0),
        (shape((count, order), bf16),),
        [SMEM, VMEM, VMEM],
        scratch,
        flops * count,
    )(scale, gram, received[0])
    far_rows = call(
        far_kernel,
        shape((count, order), bf16),
        [SMEM, SMEM] + [VMEM] * (2 + len(far_shards)),
        [packed_shape] + scratch + [pltpu.VMEM((order, order), bf16)],
        flops * count,
    )(corner, far_scale, far_here[0], local[far], *far_shards)
    if count % PAD:
        result = jnp.zeros((experts, count, order), bf16)
        for mask, rows in [(0, own_rows), (far, far_rows)] + [(m, back[m, 0]) for m in near]:
            result = lax.dynamic_update_index_in_dim(result, rows, own ^ mask, 0)
        return result
    groups = [[((0, 0), own_rows), ((far, 0), far_rows)], []]
    for (mask, index), value in back.items():
        groups[index == lots - 1].append(((mask, index * lot), value))
    result = None
    for group in groups:
        earlier = [] if result is None else [result]
        result = pl.pallas_call(
            functools.partial(place_kernel, [move for move, _ in group], len(earlier)),
            name="place",
            out_shape=shape((experts, count, order), bf16),
            in_specs=[SMEM]
            + [pl.BlockSpec(memory_space=pltpu.HBM)] * len(earlier)
            + [VMEM] * len(group),
            out_specs=pl.BlockSpec(memory_space=pltpu.HBM),
            scratch_shapes=[pltpu.SemaphoreType.DMA((len(group),))],
            input_output_aliases={1: 0} if earlier else {},
            cost_estimate=pl.CostEstimate(flops=1 << 20, bytes_accessed=1 << 20, transcendentals=0),
            compiler_params=pltpu.CompilerParams(vmem_limit_bytes=LIMIT),
        )(where, *earlier, *[value for _, value in group])
    return result


def lots_of(count):
    return 1 if count % (2 * PAD) else 2


def gather_turns(parts):
    return list(range(parts - 1, 0, -1))


def solution(mesh):
    experts, pieces = mesh.shape["expert"], mesh.shape["fsdp"]

    def body(momentum, spectral_sq):
        height = momentum.shape[1] * experts * pieces
        return on_device(experts, pieces, height, momentum, spectral_sq)

    def run(momentum, spectral_sq):
        step = jax.shard_map(
            body,
            mesh=mesh,
            in_specs=(P(None, ("fsdp", "expert"), None), P("expert")),
            out_specs=P(None, ("fsdp", "expert"), None),
            check_vma=False,
        )
        return step(momentum, spectral_sq)

    return run
```
